32 devices in a mesh: src: 16 (over z, y, core), tgt: 2 (over x).
Axes of the slice: x: 2, y: 2, z: 4, core: 2. Of those that a mesh axis runs over, the one named last changes fastest.
Arguments:
- positions: float32 [3, 4096], P(None, ('src', 'tgt')), may hold values from -1.3 to 1.3, as said below
- areas: float32 [4096], P(('src', 'tgt')), may hold values from 0.25 to 4
- right_side: float32 [3, 4096], P(None, ('src', 'tgt')), may hold values from -6 to 6
Outputs:
- solution_field: float32 [3, 4096], P(None, ('src', 'tgt'))
- residual: float32 [3, 4096], P(None, ('src', 'tgt'))
- hessenberg: float32 [5, 4], replicated
The draws below stay inside these ranges and needn't reach their ends.
Inputs may be any that keep to these rules, and one draw needn't show every extreme that they name: positions lie on a sphere of radius 1 or an ellipsoid centred at the anchor with semi-axes between 0.7 and 1.3, with no locality in how panels are assigned to devices.
All inputs are finite; a program needn't handle non-finite values.
Results may differ from the reference program's by a relative error of at most 0.0003.
Values sent between devices are 32-bit elements.
A program may use at most 64 MiB of HBM per device.

```python
import math
import jax
import jax.numpy as jnp
from jax import lax

ITERS = 4
PANELS = 4096


def draw_positions(key, part):
    points = jax.random.normal(key, (3, PANELS), jnp.float32)
    sphere = points / jnp.linalg.norm(points, axis=0, keepdims=True)
    return sphere


def level_of(key, dims, shards, low, largest):
    level = 1.0
    for position, parts in shards:
        heights = jax.random.uniform(jax.random.fold_in(jax.random.fold_in(key, 6), position), (parts,), jnp.float32, low / len(shards), largest / len(shards))
        level = level * jnp.repeat(jnp.exp(heights), dims[position] // parts).reshape((-1,) + (1,) * (len(dims) - 1 - position))
    return level


def bell_draw(rng, shape, scale, bound, pieces=(), held_as=jnp.bfloat16):
    drawn = jax.random.normal(rng, shape, jnp.float32) * scale
    if len(pieces) > 0:
        drawn = level_of(rng, shape, pieces, -0.22, 0.18) * drawn
    return jnp.clip(drawn, min=-bound, max=bound).astype(held_as)


def setup_inputs(seed: int = 0) -> dict:
    streams_of = jax.random.split(jax.random.key(seed), 4)
    positions = draw_positions(jax.random.fold_in(streams_of[3], 71), 0)
    areas = jnp.clip(jnp.exp(math.log(4.0) - 2.7725887 * jax.random.uniform(streams_of[1], (PANELS,), jnp.float32) ** level_of(streams_of[1], (PANELS,), ((0, 32),), -0.2, 0.2)), 0.25, 4.0)
    right_side = bell_draw(streams_of[2], (3, PANELS), 1.0, 6.0, ((1, 32),), jnp.float32)
    return dict(positions=positions, areas=areas, right_side=right_side)


soften = 0.0025

def stokes_block(targets, sources, densities):
    offset = targets[:, :, None] - sources[:, None, :]
    square = lax.optimization_barrier(jnp.sum(offset * offset, axis=0)) + soften
    factor = square ** (-1.5)
    projected = lax.optimization_barrier(jnp.sum(offset * densities[:, None, :], axis=0))
    return lax.optimization_barrier(jnp.sum(factor[None] * ((square + soften)[None] * densities[:, None, :] + offset * projected[None]), axis=2))

def apply_operator(vector, positions, areas):
    weighted = vector * (areas * PANELS ** (-0.5))[None, :]
    row_block = math.gcd(PANELS, 256)
    blocks = PANELS // row_block
    target_blocks = positions.reshape(3, blocks, row_block).transpose(1, 0, 2)

    def one_block(targets):
        return stokes_block(targets, positions, weighted)
    induced = lax.map(one_block, target_blocks)
    return vector + induced.transpose(1, 0, 2).reshape(3, PANELS)

def least_squares(hessenberg, initial):
    columns = hessenberg.shape[1]
    triangle = hessenberg
    target = jnp.zeros((hessenberg.shape[0],), jnp.float32).at[0].set(initial)
    for column in range(columns):
        leading = triangle[column, column]
        second = triangle[column + 1, column]
        radius = jnp.sqrt(leading * leading + second * second)
        cosine = leading / radius
        sine_value = second / radius
        row_top = triangle[column]
        row_low = triangle[column + 1]
        triangle = triangle.at[column].set(cosine * row_top + sine_value * row_low)
        triangle = triangle.at[column + 1].set(cosine * row_low - sine_value * row_top)
        target_top = target[column]
        target_low = target[column + 1]
        target = target.at[column].set(cosine * target_top + sine_value * target_low)
        target = target.at[column + 1].set(cosine * target_low - sine_value * target_top)
    solution = jnp.zeros((columns,), jnp.float32)
    for row_index in reversed(range(columns)):
        partial_sum = jnp.sum(triangle[row_index, row_index + 1:columns] * solution[row_index + 1:columns])
        solution = solution.at[row_index].set((target[row_index] - partial_sum) / triangle[row_index, row_index])
    return solution

def reference(positions, areas, right_side):
    initial = jnp.sqrt(jnp.sum(right_side * right_side))
    krylov_basis = [right_side / initial]
    hessenberg = jnp.zeros((ITERS + 1, ITERS), jnp.float32)
    for iteration in range(ITERS):
        applied = apply_operator(krylov_basis[iteration], positions, areas)
        stacked = jnp.stack(krylov_basis)
        projections = lax.optimization_barrier(jnp.sum(stacked * applied[None], axis=(1, 2)))
        remainder = applied - lax.optimization_barrier(jnp.sum(projections[:, None, None] * stacked, axis=0))
        height = jnp.sqrt(jnp.sum(remainder * remainder))
        hessenberg = hessenberg.at[:iteration + 1, iteration].set(projections)
        hessenberg = hessenberg.at[iteration + 1, iteration].set(height)
        krylov_basis.append(remainder / height)
    coefficients = least_squares(hessenberg, initial)
    stacked = jnp.stack(krylov_basis)
    solution_field = lax.optimization_barrier(jnp.sum(coefficients[:, None, None] * stacked[:ITERS], axis=0))
    misfit = -lax.optimization_barrier(jnp.sum(hessenberg * coefficients[None, :], axis=1))
    misfit = misfit.at[0].add(initial)
    residual = lax.optimization_barrier(jnp.sum(misfit[:, None, None] * stacked, axis=0))
    return (solution_field, residual, hessenberg)
```

```python
import functools

import jax
import jax.numpy as jnp
from jax import lax
from jax.experimental import pallas as pl
from jax.experimental.pallas import tpu as pltpu
from jax.sharding import PartitionSpec as P

ITERS = 4
soften = 0.0025
MESH = pl.DeviceIdType.MESH
CACHE_BYTES = 24 * 2**20


def total(value):
    while value.ndim > 2:
        value = jnp.sum(value, axis=0)
    return jnp.sum(jnp.sum(value, axis=0, keepdims=True), axis=1, keepdims=True)


def pair_tables(targets, sources):
    r = [t - s for t, s in zip(targets, sources)]
    square = r[0] * r[0] + r[1] * r[1] + r[2] * r[2] + soften
    inverse = lax.rsqrt(square)
    factor = inverse * inverse * inverse
    root = inverse * inverse * lax.rsqrt(inverse)
    near = factor * (square + soften)
    return near, [root * c for c in r]


def flip(index, mask, bits):
    out = index
    for b in range(bits):
        if isinstance(mask, int):
            chosen = (mask >> b) & 1
            if not chosen:
                continue
        else:
            chosen = lax.rem(lax.div(mask, 1 << b), 2)
        mine = lax.rem(lax.div(index, 1 << b), 2)
        out = out + chosen * (1 - 2 * mine) * (1 << b)
    return out


def kernel(
    S, T, L, cached, group,
    pos_ref, area_ref, rhs_ref, sol_ref, res_ref, hess_ref,
    geo, wbuf, basis, acc, tcol, tables, send_sem, recv_sem,
):
    D = S * T
    bits = D.bit_length() - 1
    me = lax.axis_index("src") * T + lax.axis_index("tgt")
    group_bits = group.bit_length() - 1
    low_me = [flip(lax.rem(me, group), j, group_bits) for j in range(group)]
    high_me = lax.div(me, group)

    def coords(p):
        return (lax.div(p, T), lax.rem(p, T))

    barrier = pltpu.get_barrier_semaphore()

    def greet(s, unused):
        high = flip(high_me, s, bits - group_bits)
        for j in range(group):
            p = high * group + low_me[j]

            def signal():
                pl.semaphore_signal(barrier, inc=1, device_id=coords(p), device_id_type=MESH)

            if j == 0:
                pl.when(s > 0)(signal)
            else:
                signal()
        return unused

    lax.fori_loop(0, D // group, greet, 0)

    coefficient = float(L * D) ** (-0.5)
    geo[me, 0:3, :] = pos_ref[...]
    geo[me, 3:4, :] = area_ref[...] * coefficient
    geo[me, 4:7, :] = rhs_ref[...]
    geo[me, 7:8, :] = jnp.zeros((1, L), jnp.float32)
    for a in range(3):
        tcol[a] = jnp.broadcast_to(pos_ref[a : a + 1, :], (L, L)).T
    pl.semaphore_wait(barrier, D - 1)

    def copy(buffer, phase, source, dest):
        return pltpu.make_async_remote_copy(
            src_ref=buffer.at[source],
            dst_ref=buffer.at[source],
            send_sem=send_sem.at[phase],
            recv_sem=recv_sem.at[phase, source],
            device_id=coords(dest),
            device_id_type=MESH,
        )

    def send_all(buffer, phase):
        def step(i, unused):
            high = flip(high_me, D // group - 1 - i, bits - group_bits)
            for j in reversed(range(group)):
                copy(buffer, phase, me, high * group + low_me[j]).start()
            return unused

        lax.fori_loop(0, D // group - 1, step, 0)
        for j in reversed(range(1, group)):
            copy(buffer, phase, me, high_me * group + low_me[j]).start()

    rows = 32 if L % 32 == 0 else L

    def blocks_of(high):
        return [high * group + low_me[j] for j in range(group)]

    def absorb(high, density, first, fresh):
        ps = blocks_of(high)
        qs = [density(p) * geo[p, 3:4, :] for p in ps]
        for r0 in range(0, L, rows):
            span = pl.ds(r0, rows)
            sums = None if fresh else [acc[a, span, :] for a in range(3)]
            for p, q in zip(ps, qs):
                q = [q[a : a + 1, :] for a in range(3)]
                if cached and not first:
                    near = tables[0, p, span, :]
                    g = [tables[1 + a, p, span, :] for a in range(3)]
                else:
                    near, g = pair_tables(
                        [tcol[a, span, :] for a in range(3)], [geo[p, a : a + 1, :] for a in range(3)]
                    )
                    if cached:
                        tables[0, p, span, :] = near
                        for a in range(3):
                            tables[1 + a, p, span, :] = g[a]
                along = g[0] * q[0] + g[1] * q[1] + g[2] * q[2]
                terms = [near * q[a] + g[a] * along for a in range(3)]
                sums = terms if sums is None else [x + y for x, y in zip(sums, terms)]
            for a in range(3):
                acc[a, span, :] = sums[a]

    def receive(buffer, phase, density, first, compute):
        for j in range(1, group):
            p = high_me * group + low_me[j]
            copy(buffer, phase, p, p).wait_recv()
        if compute:
            absorb(high_me, density, first, True)

        def step(s, unused):
            high = flip(high_me, s, bits - group_bits)
            for j in range(group):
                p = high * group + low_me[j]
                copy(buffer, phase, p, p).wait_recv()
            if compute:
                absorb(high, density, first, False)
            return unused

        lax.fori_loop(1, D // group, step, 0)
        if compute:
            return jnp.concatenate(
                [jnp.sum(acc[a].T, axis=0, keepdims=True) for a in range(3)], axis=0
            )
        return None

    send_all(geo, 0)
    induced = receive(geo, 0, lambda p: geo[p, 4:7, :], True, True)
    own = rhs_ref[...] + induced
    wbuf[0, me] = own
    send_all(wbuf.at[0], 1)

    full = geo[:, 4:7, :]
    initial = jnp.sqrt(total(full * full))
    scale = 1.0 / initial
    basis[0] = full * scale
    mine = [rhs_ref[...] * scale]

    zero = jnp.zeros((1, 1), jnp.float32)
    hess = [[zero] * ITERS for _ in range(ITERS + 1)]
    triangle = [[zero] * ITERS for _ in range(ITERS)]
    target = [initial] + [zero] * ITERS
    rotations = []
    applied_mine = []
    for k in range(ITERS):
        last = k == ITERS - 1
        induced = receive(wbuf.at[k], k + 1, lambda p: wbuf[k, p], False, not last)
        applied = wbuf[k] * scale
        applied_mine.append(own * scale)
        projections = [total(basis[i] * applied) for i in range(k + 1)]
        if not last:
            own = (own + induced) * scale
            for i in range(k + 1):
                own = own - projections[i] * applied_mine[i]
            wbuf[k + 1, me] = own
            send_all(wbuf.at[k + 1], k + 2)
        remainder = applied
        removed = projections[0] * basis[0]
        removed_mine = projections[0] * mine[0]
        for i in range(1, k + 1):
            removed = removed + projections[i] * basis[i]
            removed_mine = removed_mine + projections[i] * mine[i]
        remainder = applied - removed
        height = jnp.sqrt(total(remainder * remainder))
        scale = 1.0 / height
        if not last:
            basis[k + 1] = remainder * scale
        mine.append((applied_mine[k] - removed_mine) * scale)
        for i in range(k + 1):
            hess[i][k] = projections[i]
        hess[k + 1][k] = height
        column = list(projections)
        for i, (cosine, sine) in enumerate(rotations):
            top, low = column[i], column[i + 1]
            column[i] = cosine * top + sine * low
            column[i + 1] = cosine * low - sine * top
        leading = column[k]
        radius = jnp.sqrt(leading * leading + height * height)
        cosine, sine = leading / radius, height / radius
        rotations.append((cosine, sine))
        column[k] = cosine * leading + sine * height
        for i in range(k + 1):
            triangle[i][k] = column[i]
        top = target[k]
        target[k] = cosine * top
        target[k + 1] = -sine * top

    y = [None] * ITERS
    for i in reversed(range(ITERS)):
        left = target[i]
        for j in range(i + 1, ITERS):
            left = left - triangle[i][j] * y[j]
        y[i] = left / triangle[i][i]
    solution_field = y[0] * mine[0]
    for i in range(1, ITERS):
        solution_field = solution_field + y[i] * mine[i]
    sol_ref[...] = solution_field
    residual = None
    for i in range(ITERS + 1):
        gap = initial if i == 0 else zero
        for j in range(max(i - 1, 0), ITERS):
            gap = gap - hess[i][j] * y[j]
        term = gap * mine[i]
        residual = term if residual is None else residual + term
    res_ref[...] = residual
    row = lax.broadcasted_iota(jnp.int32, (ITERS + 1, ITERS), 0)
    col = lax.broadcasted_iota(jnp.int32, (ITERS + 1, ITERS), 1)
    table = jnp.zeros((ITERS + 1, ITERS), jnp.float32)
    for k in range(ITERS):
        for i in range(k + 2):
            table = jnp.where((row == i) & (col == k), hess[i][k], table)
    hess_ref[...] = table

    for phase in range(ITERS + 1):
        buffer = geo if phase == 0 else wbuf.at[phase - 1]
        everyone = buffer.at[pl.ds(0, D - 1)]
        pltpu.make_async_remote_copy(
            src_ref=everyone,
            dst_ref=everyone,
            send_sem=send_sem.at[phase],
            recv_sem=recv_sem.at[phase, me],
            device_id=coords(me),
            device_id_type=MESH,
        ).wait_send()


def local(S, T, positions, areas, right_side):
    L = positions.shape[1]
    D = S * T
    group = 4
    cached = 4 * D * L * L * 4 <= CACHE_BYTES
    f32 = jnp.float32
    return pl.pallas_call(
        functools.partial(kernel, S, T, L, cached, group),
        out_shape=(
            jax.ShapeDtypeStruct((3, L), f32),
            jax.ShapeDtypeStruct((3, L), f32),
            jax.ShapeDtypeStruct((ITERS + 1, ITERS), f32),
        ),
        in_specs=[pl.BlockSpec(memory_space=pltpu.VMEM)] * 3,
        out_specs=(pl.BlockSpec(memory_space=pltpu.VMEM),) * 3,
        scratch_shapes=[
            pltpu.VMEM((D, 8, L), f32),
            pltpu.VMEM((ITERS, D, 3, L), f32),
            pltpu.VMEM((ITERS, D, 3, L), f32),
            pltpu.VMEM((3, L, L), f32),
            pltpu.VMEM((3, L, L), f32),
            pltpu.VMEM((4, D, L, L) if cached else (1, 1, 8, 128), f32),
            pltpu.SemaphoreType.DMA((ITERS + 1,)),
            pltpu.SemaphoreType.DMA((ITERS + 1, D)),
        ],
        compiler_params=pltpu.CompilerParams(
            collective_id=0, has_side_effects=True, vmem_limit_bytes=48 * 2**20
        ),
    )(positions, areas.reshape(1, L), right_side)


def solution(mesh):
    S, T = mesh.shape["src"], mesh.shape["tgt"]
    return jax.shard_map(
        functools.partial(local, S, T),
        mesh=mesh,
        in_specs=(P(None, ("src", "tgt")), P(("src", "tgt")), P(None, ("src", "tgt"))),
        out_specs=(P(None, ("src", "tgt")), P(None, ("src", "tgt")), P()),
        check_vma=False,
    )
```

```python
import functools

import jax
import jax.numpy as jnp
from jax import lax
from jax.experimental import pallas as pl
from jax.experimental.pallas import tpu as pltpu
from jax.sharding import PartitionSpec as P

ITERS = 4
soften = 0.0025
MESH = pl.DeviceIdType.MESH
CACHE_BYTES = 24 * 2**20


def total(value):
    while value.ndim > 2:
        value = jnp.sum(value, axis=0)
    return jnp.sum(jnp.sum(value, axis=0, keepdims=True), axis=1, keepdims=True)


def pair_tables(targets, sources):
    r = [t - s for t, s in zip(targets, sources)]
    square = r[0] * r[0] + r[1] * r[1] + r[2] * r[2] + soften
    inverse = lax.rsqrt(square)
    factor = inverse * inverse * inverse
    root = inverse * inverse * lax.rsqrt(inverse)
    near = factor * (square + soften)
    return near, [root * c for c in r]


def flip(index, mask, bits):
    out = index
    for b in range(bits):
        if isinstance(mask, int):
            chosen = (mask >> b) & 1
            if not chosen:
                continue
        else:
            chosen = lax.rem(lax.div(mask, 1 << b), 2)
        mine = lax.rem(lax.div(index, 1 << b), 2)
        out = out + chosen * (1 - 2 * mine) * (1 << b)
    return out


def kernel(
    S, T, L, cached, group,
    pos_in, area_in, rhs_in, out_ref,
    pos_ref, area_ref, rhs_ref, geo, wbuf, whole, basis, acc, tcol, tables,
    load_sem, send_sem, recv_sem,
):
    D = S * T
    bits = D.bit_length() - 1
    me = lax.axis_index("src") * T + lax.axis_index("tgt")
    group_bits = group.bit_length() - 1
    low_me = [flip(lax.rem(me, group), j, group_bits) for j in range(group)]
    high_me = lax.div(me, group)

    def coords(p):
        return (lax.div(p, T), lax.rem(p, T))

    barrier = pltpu.get_barrier_semaphore()

    def greet(s, unused):
        high = flip(high_me, s, bits - group_bits)
        for j in range(group):
            p = high * group + low_me[j]

            def signal():
                pl.semaphore_signal(barrier, inc=1, device_id=coords(p), device_id_type=MESH)

            if j == 0:
                pl.when(s > 0)(signal)
            else:
                signal()
        return unused

    lax.fori_loop(0, D // group, greet, 0)
    loads = [
        pltpu.make_async_copy(x, y, load_sem.at[i])
        for i, (x, y) in enumerate([(pos_in, pos_ref), (area_in, area_ref), (rhs_in, rhs_ref)])
    ]
    for load in loads:
        load.start()
    for load in loads:
        load.wait()

    coefficient = float(L * D) ** (-0.5)
    geo[me, 0:3, :] = pos_ref[...]
    geo[me, 3:4, :] = area_ref[...] * coefficient
    geo[me, 4:7, :] = rhs_ref[...]
    geo[me, 7:8, :] = jnp.zeros((1, L), jnp.float32)
    for a in range(3):
        tcol[a] = jnp.broadcast_to(pos_ref[a : a + 1, :], (L, L)).T
    pl.semaphore_wait(barrier, D - 1)

    def copy(buffer, phase, source, dest):
        return pltpu.make_async_remote_copy(
            src_ref=buffer.at[source],
            dst_ref=buffer.at[source],
            send_sem=send_sem.at[phase],
            recv_sem=recv_sem.at[phase, source],
            device_id=coords(dest),
            device_id_type=MESH,
        )

    def send_all(buffer, phase):
        def step(i, unused):
            high = flip(high_me, D // group - 1 - i, bits - group_bits)
            for j in reversed(range(group)):
                copy(buffer, phase, me, high * group + low_me[j]).start()
            return unused

        lax.fori_loop(0, D // group - 1, step, 0)
        for j in reversed(range(1, group)):
            copy(buffer, phase, me, high_me * group + low_me[j]).start()

    rows = 32 if L % 32 == 0 else L

    def blocks_of(high):
        return [high * group + low_me[j] for j in range(group)]

    def absorb(high, density, first, fresh):
        ps = blocks_of(high)
        qs = [density(p) * geo[p, 3:4, :] for p in ps]
        for r0 in range(0, L, rows):
            span = pl.ds(r0, rows)
            sums = None if fresh else [acc[a, span, :] for a in range(3)]
            for p, q in zip(ps, qs):
                q = [q[a : a + 1, :] for a in range(3)]
                if cached and not first:
                    near = tables[0, p, span, :]
                    g = [tables[1 + a, p, span, :] for a in range(3)]
                else:
                    near, g = pair_tables(
                        [tcol[a, span, :] for a in range(3)], [geo[p, a : a + 1, :] for a in range(3)]
                    )
                    if cached:
                        tables[0, p, span, :] = near
                        for a in range(3):
                            tables[1 + a, p, span, :] = g[a]
                along = g[0] * q[0] + g[1] * q[1] + g[2] * q[2]
                terms = [near * q[a] + g[a] * along for a in range(3)]
                sums = terms if sums is None else [x + y for x, y in zip(sums, terms)]
            for a in range(3):
                acc[a, span, :] = sums[a]

    def receive(buffer, phase, density, first, compute):
        for j in range(1, group):
            p = high_me * group + low_me[j]
            copy(buffer, phase, p, p).wait_recv()
        if compute:
            absorb(high_me, density, first, True)

        def step(s, unused):
            high = flip(high_me, s, bits - group_bits)
            for j in range(group):
                p = high * group + low_me[j]
                copy(buffer, phase, p, p).wait_recv()
            if compute:
                absorb(high, density, first, False)
            return unused

        lax.fori_loop(1, D // group, step, 0)
        if compute:
            return jnp.concatenate(
                [jnp.sum(acc[a].T, axis=0, keepdims=True) for a in range(3)], axis=0
            )
        return None

    send_all(geo, 0)
    induced = receive(geo, 0, lambda p: geo[p, 4:7, :], True, True)
    own = rhs_ref[...] + induced
    wbuf[0, me] = own
    send_all(wbuf.at[0], 1)

    full = geo[:, 4:7, :]
    initial = jnp.sqrt(total(full * full))
    scale = 1.0 / initial
    basis[0] = full * scale
    mine = [rhs_ref[...] * scale]

    zero = jnp.zeros((1, 1), jnp.float32)
    hess = [[zero] * ITERS for _ in range(ITERS + 1)]
    triangle = [[zero] * ITERS for _ in range(ITERS)]
    target = [initial] + [zero] * ITERS
    rotations = []
    applied_mine = []
    sent = [own]
    for k in range(ITERS):
        last = k == ITERS - 1
        induced = receive(wbuf.at[k], k + 1, lambda p: wbuf[k, p], False, not last)
        if not last:
            own = own + induced
            for i in range(k):
                own = own - hess[i][k - 1] * sent[i + 1]
            own = own * scale
            wbuf[k + 1, me] = own
            send_all(wbuf.at[k + 1], k + 2)
            sent.append(own)
        applied = wbuf[k]
        mine_now = wbuf[k, me]
        for i in range(k):
            applied = applied - hess[i][k - 1] * whole[i]
            mine_now = mine_now - hess[i][k - 1] * applied_mine[i]
        applied = applied * scale
        applied_mine.append(mine_now * scale)
        if not last:
            whole[k] = applied
        projections = [total(basis[i] * applied) for i in range(k + 1)]
        removed = projections[0] * basis[0]
        removed_mine = projections[0] * mine[0]
        for i in range(1, k + 1):
            removed = removed + projections[i] * basis[i]
            removed_mine = removed_mine + projections[i] * mine[i]
        remainder = applied - removed
        height = jnp.sqrt(total(remainder * remainder))
        scale = 1.0 / height
        if not last:
            basis[k + 1] = remainder * scale
        mine.append((applied_mine[k] - removed_mine) * scale)
        for i in range(k + 1):
            hess[i][k] = projections[i]
        hess[k + 1][k] = height
        column = list(projections)
        for i, (cosine, sine) in enumerate(rotations):
            top, low = column[i], column[i + 1]
            column[i] = cosine * top + sine * low
            column[i + 1] = cosine * low - sine * top
        leading = column[k]
        radius = jnp.sqrt(leading * leading + height * height)
        cosine, sine = leading / radius, height / radius
        rotations.append((cosine, sine))
        column[k] = cosine * leading + sine * height
        for i in range(k + 1):
            triangle[i][k] = column[i]
        top = target[k]
        target[k] = cosine * top
        target[k + 1] = -sine * top

    y = [None] * ITERS
    for i in reversed(range(ITERS)):
        left = target[i]
        for j in range(i + 1, ITERS):
            left = left - triangle[i][j] * y[j]
        y[i] = left / triangle[i][i]
    solution_field = y[0] * mine[0]
    for i in range(1, ITERS):
        solution_field = solution_field + y[i] * mine[i]
    out_ref[0:3, :] = solution_field
    residual = None
    for i in range(ITERS + 1):
        gap = initial if i == 0 else zero
        for j in range(max(i - 1, 0), ITERS):
            gap = gap - hess[i][j] * y[j]
        term = gap * mine[i]
        residual = term if residual is None else residual + term
    out_ref[8:11, :] = residual
    row = lax.broadcasted_iota(jnp.int32, (8, L), 0)
    col = lax.broadcasted_iota(jnp.int32, (8, L), 1)
    table = jnp.zeros((8, L), jnp.float32)
    for k in range(ITERS):
        for i in range(k + 2):
            table = jnp.where((row == k) & (col == i), hess[i][k], table)
    out_ref[16:24, :] = table

    for phase in range(ITERS + 1):
        buffer = geo if phase == 0 else wbuf.at[phase - 1]
        everyone = buffer.at[pl.ds(0, D - 1)]
        pltpu.make_async_remote_copy(
            src_ref=everyone,
            dst_ref=everyone,
            send_sem=send_sem.at[phase],
            recv_sem=recv_sem.at[phase, me],
            device_id=coords(me),
            device_id_type=MESH,
        ).wait_send()


def unpack(packed_ref, sol_ref, res_ref, hess_ref):
    sol_ref[...] = packed_ref[0:3, :]
    res_ref[...] = packed_ref[8:11, :]
    hess_ref[...] = packed_ref[16 : 16 + ITERS, 0 : ITERS + 1]


def local(S, T, positions, areas, right_side):
    L = positions.shape[1]
    D = S * T
    group = 4
    cached = 4 * D * L * L * 4 <= CACHE_BYTES
    f32 = jnp.float32
    vmem = pl.BlockSpec(memory_space=pltpu.VMEM)
    packed = pl.pallas_call(
        functools.partial(kernel, S, T, L, cached, group),
        out_shape=jax.ShapeDtypeStruct((24, L), f32),
        in_specs=[pl.BlockSpec(memory_space=pltpu.HBM)] * 3,
        out_specs=vmem,
        scratch_shapes=[
            pltpu.VMEM((3, L), f32),
            pltpu.VMEM((1, L), f32),
            pltpu.VMEM((3, L), f32),
            pltpu.VMEM((D, 8, L), f32),
            pltpu.VMEM((ITERS, D, 3, L), f32),
            pltpu.VMEM((ITERS - 1, D, 3, L), f32),
            pltpu.VMEM((ITERS, D, 3, L), f32),
            pltpu.VMEM((3, L, L), f32),
            pltpu.VMEM((3, L, L), f32),
            pltpu.VMEM((4, D, L, L) if cached else (1, 1, 8, 128), f32),
            pltpu.SemaphoreType.DMA((3,)),
            pltpu.SemaphoreType.DMA((ITERS + 1,)),
            pltpu.SemaphoreType.DMA((ITERS + 1, D)),
        ],
        compiler_params=pltpu.CompilerParams(
            collective_id=0, has_side_effects=True, vmem_limit_bytes=67043328
        ),
    )(positions, areas.reshape(1, L), right_side)
    field, residual, columns = pl.pallas_call(
        unpack,
        out_shape=(
            jax.ShapeDtypeStruct((3, L), f32),
            jax.ShapeDtypeStruct((3, L), f32),
            jax.ShapeDtypeStruct((ITERS, ITERS + 1), f32),
        ),
        in_specs=[vmem],
        out_specs=(vmem,) * 3,
        compiler_params=pltpu.CompilerParams(vmem_limit_bytes=2**20),
    )(packed)
    return field, residual, columns.T


def solution(mesh):
    S, T = mesh.shape["src"], mesh.shape["tgt"]
    return jax.shard_map(
        functools.partial(local, S, T),
        mesh=mesh,
        in_specs=(P(None, ("src", "tgt")), P(("src", "tgt")), P(None, ("src", "tgt"))),
        out_specs=(P(None, ("src", "tgt")), P(None, ("src", "tgt")), P()),
        check_vma=False,
    )
```

```python
import functools

import jax
import jax.numpy as jnp
from jax import lax
from jax.experimental import pallas as pl
from jax.experimental.pallas import tpu as pltpu
from jax.sharding import PartitionSpec as P

ITERS = 4
soften = 0.0025
MESH = pl.DeviceIdType.MESH
CACHE_BYTES = 24 * 2**20


def total(value):
    while value.ndim > 2:
        value = jnp.sum(value, axis=0)
    return jnp.sum(jnp.sum(value, axis=0, keepdims=True), axis=1, keepdims=True)


def pair_tables(targets, sources):
    r = [t - s for t, s in zip(targets, sources)]
    square = r[0] * r[0] + r[1] * r[1] + r[2] * r[2] + soften
    inverse = lax.rsqrt(square)
    factor = inverse * inverse * inverse
    root = inverse * inverse * lax.rsqrt(inverse)
    near = factor * (square + soften)
    return near, [root * c for c in r]


def pair_terms(targets, sources):
    r = [t - s for t, s in zip(targets, sources)]
    square = r[0] * r[0] + r[1] * r[1] + r[2] * r[2] + soften
    inverse = lax.rsqrt(square)
    factor = inverse * inverse * inverse
    return factor * (square + soften), factor, r


def flip(index, mask, bits):
    out = index
    for b in range(bits):
        if isinstance(mask, int):
            chosen = (mask >> b) & 1
            if not chosen:
                continue
        else:
            chosen = lax.rem(lax.div(mask, 1 << b), 2)
        mine = lax.rem(lax.div(index, 1 << b), 2)
        out = out + chosen * (1 - 2 * mine) * (1 << b)
    return out


def kernel(
    S, T, L, cached, group,
    pos_in, area_in, rhs_in, out_ref,
    pos_ref, area_ref, rhs_ref, geo, wbuf, whole, basis, acc, tcol, tables,
    load_sem, send_sem, recv_sem,
):
    D = S * T
    bits = D.bit_length() - 1
    me = lax.axis_index("src") * T + lax.axis_index("tgt")
    group_bits = group.bit_length() - 1
    low_me = [flip(lax.rem(me, group), j, group_bits) for j in range(group)]
    high_me = lax.div(me, group)

    def coords(p):
        return (lax.div(p, T), lax.rem(p, T))

    barrier = pltpu.get_barrier_semaphore()

    def greet(s, unused):
        high = flip(high_me, s, bits - group_bits)
        for j in range(group):
            p = high * group + low_me[j]

            def signal():
                pl.semaphore_signal(barrier, inc=1, device_id=coords(p), device_id_type=MESH)

            if j == 0:
                pl.when(s > 0)(signal)
            else:
                signal()
        return unused

    lax.fori_loop(0, D // group, greet, 0)
    loads = [
        pltpu.make_async_copy(x, y, load_sem.at[i])
        for i, (x, y) in enumerate([(pos_in, pos_ref), (area_in, area_ref), (rhs_in, rhs_ref)])
    ]
    for load in loads:
        load.start()
    for load in loads:
        load.wait()

    coefficient = float(L * D) ** (-0.5)
    geo[me, 0:3, :] = pos_ref[...]
    geo[me, 3:4, :] = area_ref[...] * coefficient
    geo[me, 4:7, :] = rhs_ref[...]
    geo[me, 7:8, :] = jnp.zeros((1, L), jnp.float32)
    for a in range(3):
        tcol[a] = jnp.broadcast_to(pos_ref[a : a + 1, :], (L, L)).T
    pl.semaphore_wait(barrier, D - 1)

    def copy(buffer, phase, source, dest):
        return pltpu.make_async_remote_copy(
            src_ref=buffer.at[source],
            dst_ref=buffer.at[source],
            send_sem=send_sem.at[phase],
            recv_sem=recv_sem.at[phase, source],
            device_id=coords(dest),
            device_id_type=MESH,
        )

    def send_all(buffer, phase):
        def step(i, unused):
            high = flip(high_me, D // group - 1 - i, bits - group_bits)
            for j in reversed(range(group)):
                copy(buffer, phase, me, high * group + low_me[j]).start()
            return unused

        lax.fori_loop(0, D // group - 1, step, 0)
        for j in reversed(range(1, group)):
            copy(buffer, phase, me, high_me * group + low_me[j]).start()

    rows = 32 if L % 32 == 0 else L

    def blocks_of(high):
        return [high * group + low_me[j] for j in range(group)]

    def absorb(high, density, first, fresh):
        ps = blocks_of(high)
        qs = [density(p) * geo[p, 3:4, :] for p in ps]
        for r0 in range(0, L, rows):
            span = pl.ds(r0, rows)
            sums = None if fresh else [acc[a, span, :] for a in range(3)]
            for p, q in zip(ps, qs):
                q = [q[a : a + 1, :] for a in range(3)]
                if cached and not first:
                    near = tables[0, p, span, :]
                    g = [tables[1 + a, p, span, :] for a in range(3)]
                else:
                    near, factor, g = pair_terms(
                        [tcol[a, span, :] for a in range(3)], [geo[p, a : a + 1, :] for a in range(3)]
                    )
                along = g[0] * q[0] + g[1] * q[1] + g[2] * q[2]
                if first or not cached:
                    along = along * factor
                terms = [near * q[a] + g[a] * along for a in range(3)]
                sums = terms if sums is None else [x + y for x, y in zip(sums, terms)]
            for a in range(3):
                acc[a, span, :] = sums[a]

    def receive(buffer, phase, density, first, compute):
        for j in range(1, group):
            p = high_me * group + low_me[j]
            copy(buffer, phase, p, p).wait_recv()
        if compute:
            absorb(high_me, density, first, True)

        def step(s, unused):
            high = flip(high_me, s, bits - group_bits)
            for j in range(group):
                p = high * group + low_me[j]
                copy(buffer, phase, p, p).wait_recv()
            if compute:
                absorb(high, density, first, False)
            return unused

        lax.fori_loop(1, D // group, step, 0)
        if compute:
            return jnp.concatenate(
                [jnp.sum(acc[a].T, axis=0, keepdims=True) for a in range(3)], axis=0
            )
        return None

    send_all(geo, 0)
    induced = receive(geo, 0, lambda p: geo[p, 4:7, :], True, True)
    own = rhs_ref[...] + induced
    wbuf[0, me] = own
    send_all(wbuf.at[0], 1)

    def build(high, unused):
        for p in blocks_of(high):
            for r0 in range(0, L, rows):
                span = pl.ds(r0, rows)
                near, g = pair_tables(
                    [tcol[a, span, :] for a in range(3)], [geo[p, a : a + 1, :] for a in range(3)]
                )
                tables[0, p, span, :] = near
                for a in range(3):
                    tables[1 + a, p, span, :] = g[a]
        return unused

    if cached:
        lax.fori_loop(0, D // group, build, 0)

    full = geo[:, 4:7, :]
    initial = jnp.sqrt(total(full * full))
    scale = 1.0 / initial
    basis[0] = full * scale
    mine = [rhs_ref[...] * scale]

    zero = jnp.zeros((1, 1), jnp.float32)
    hess = [[zero] * ITERS for _ in range(ITERS + 1)]
    triangle = [[zero] * ITERS for _ in range(ITERS)]
    target = [initial] + [zero] * ITERS
    rotations = []
    applied_mine = []
    sent = [own]
    for k in range(ITERS):
        last = k == ITERS - 1
        induced = receive(wbuf.at[k], k + 1, lambda p: wbuf[k, p], False, not last)
        if not last:
            own = own + induced
            for i in range(k):
                own = own - hess[i][k - 1] * sent[i + 1]
            own = own * scale
            wbuf[k + 1, me] = own
            send_all(wbuf.at[k + 1], k + 2)
            sent.append(own)
        applied = wbuf[k]
        mine_now = wbuf[k, me]
        for i in range(k):
            applied = applied - hess[i][k - 1] * whole[i]
            mine_now = mine_now - hess[i][k - 1] * applied_mine[i]
        applied = applied * scale
        applied_mine.append(mine_now * scale)
        if not last:
            whole[k] = applied
        projections = [total(basis[i] * applied) for i in range(k + 1)]
        removed = projections[0] * basis[0]
        removed_mine = projections[0] * mine[0]
        for i in range(1, k + 1):
            removed = removed + projections[i] * basis[i]
            removed_mine = removed_mine + projections[i] * mine[i]
        remainder = applied - removed
        height = jnp.sqrt(total(remainder * remainder))
        scale = 1.0 / height
        if not last:
            basis[k + 1] = remainder * scale
        mine.append((applied_mine[k] - removed_mine) * scale)
        for i in range(k + 1):
            hess[i][k] = projections[i]
        hess[k + 1][k] = height
        column = list(projections)
        for i, (cosine, sine) in enumerate(rotations):
            top, low = column[i], column[i + 1]
            column[i] = cosine * top + sine * low
            column[i + 1] = cosine * low - sine * top
        leading = column[k]
        radius = jnp.sqrt(leading * leading + height * height)
        cosine, sine = leading / radius, height / radius
        rotations.append((cosine, sine))
        column[k] = cosine * leading + sine * height
        for i in range(k + 1):
            triangle[i][k] = column[i]
        top = target[k]
        target[k] = cosine * top
        target[k + 1] = -sine * top

    y = [None] * ITERS
    for i in reversed(range(ITERS)):
        left = target[i]
        for j in range(i + 1, ITERS):
            left = left - triangle[i][j] * y[j]
        y[i] = left / triangle[i][i]
    solution_field = y[0] * mine[0]
    for i in range(1, ITERS):
        solution_field = solution_field + y[i] * mine[i]
    out_ref[0:3, :] = solution_field
    residual = None
    for i in range(ITERS + 1):
        gap = initial if i == 0 else zero
        for j in range(max(i - 1, 0), ITERS):
            gap = gap - hess[i][j] * y[j]
        term = gap * mine[i]
        residual = term if residual is None else residual + term
    out_ref[8:11, :] = residual
    row = lax.broadcasted_iota(jnp.int32, (8, L), 0)
    col = lax.broadcasted_iota(jnp.int32, (8, L), 1)
    table = jnp.zeros((8, L), jnp.float32)
    for k in range(ITERS):
        for i in range(k + 2):
            table = jnp.where((row == k) & (col == i), hess[i][k], table)
    out_ref[16:24, :] = table

    for phase in range(ITERS + 1):
        buffer = geo if phase == 0 else wbuf.at[phase - 1]
        everyone = buffer.at[pl.ds(0, D - 1)]
        pltpu.make_async_remote_copy(
            src_ref=everyone,
            dst_ref=everyone,
            send_sem=send_sem.at[phase],
            recv_sem=recv_sem.at[phase, me],
            device_id=coords(me),
            device_id_type=MESH,
        ).wait_send()


def unpack(packed_ref, sol_ref, res_ref, hess_ref):
    sol_ref[...] = packed_ref[0:3, :]
    res_ref[...] = packed_ref[8:11, :]
    hess_ref[...] = packed_ref[16 : 16 + ITERS, 0 : ITERS + 1]


def local(S, T, positions, areas, right_side):
    L = positions.shape[1]
    D = S * T
    group = 4
    cached = 4 * D * L * L * 4 <= CACHE_BYTES
    f32 = jnp.float32
    vmem = pl.BlockSpec(memory_space=pltpu.VMEM)
    packed = pl.pallas_call(
        functools.partial(kernel, S, T, L, cached, group),
        out_shape=jax.ShapeDtypeStruct((24, L), f32),
        in_specs=[pl.BlockSpec(memory_space=pltpu.HBM)] * 3,
        out_specs=vmem,
        scratch_shapes=[
            pltpu.VMEM((3, L), f32),
            pltpu.VMEM((1, L), f32),
            pltpu.VMEM((3, L), f32),
            pltpu.VMEM((D, 8, L), f32),
            pltpu.VMEM((ITERS, D, 3, L), f32),
            pltpu.VMEM((ITERS - 1, D, 3, L), f32),
            pltpu.VMEM((ITERS, D, 3, L), f32),
            pltpu.VMEM((3, L, L), f32),
            pltpu.VMEM((3, L, L), f32),
            pltpu.VMEM((4, D, L, L) if cached else (1, 1, 8, 128), f32),
            pltpu.SemaphoreType.DMA((3,)),
            pltpu.SemaphoreType.DMA((ITERS + 1,)),
            pltpu.SemaphoreType.DMA((ITERS + 1, D)),
        ],
        compiler_params=pltpu.CompilerParams(
            collective_id=0, has_side_effects=True, vmem_limit_bytes=67043328
        ),
    )(positions, areas.reshape(1, L), right_side)
    field, residual, columns = pl.pallas_call(
        unpack,
        out_shape=(
            jax.ShapeDtypeStruct((3, L), f32),
            jax.ShapeDtypeStruct((3, L), f32),
            jax.ShapeDtypeStruct((ITERS, ITERS + 1), f32),
        ),
        in_specs=[vmem],
        out_specs=(vmem,) * 3,
        compiler_params=pltpu.CompilerParams(vmem_limit_bytes=2**20),
    )(packed)
    return field, residual, columns.T


def solution(mesh):
    S, T = mesh.shape["src"], mesh.shape["tgt"]
    return jax.shard_map(
        functools.partial(local, S, T),
        mesh=mesh,
        in_specs=(P(None, ("src", "tgt")), P(("src", "tgt")), P(None, ("src", "tgt"))),
        out_specs=(P(None, ("src", "tgt")), P(None, ("src", "tgt")), P()),
        check_vma=False,
    )
```
